32 devices in a mesh: grp: 4 (over x, core), dev: 8 (over z, y).
Axes of the slice: x: 2, y: 2, z: 4, core: 2. Of those that a mesh axis runs over, the one named last changes fastest.
Arguments:
- sep_inv: bfloat16 [4096, 4096], P('grp', 'dev'), may hold values from -0.125 to 0.125
- panels: bfloat16 [4, 48, 2048, 128], P('grp', 'dev'), may hold values from -1.1953125 to 1.1953125
- diag_inverse: bfloat16 [4, 48, 768, 128], P('grp', 'dev'), may hold values from -6 to 6
- widths: int32 [4, 16], P('grp'), may hold values from 1 to 6, 48 in all within a row
- ancestors: int32 [4, 16, 16], P('grp'), may hold values from 0 to 31, as said below
Outputs:
- off_diag: bfloat16 [4, 48, 2048, 128], P('grp', 'dev')
- diag_panels: bfloat16 [4, 48, 768, 128], P('grp', 'dev')
The draws below stay inside these ranges and needn't reach their ends.
Inputs may be any that keep to these rules, and one draw needn't show every extreme that they name: `widths`: each row of a subtree sums to 48. `ancestors`: each supernode's list holds 16 different separator tile numbers in increasing order.
All inputs are finite; a program needn't handle non-finite values.
Results may differ from the reference program's by a relative error of at most 0.0046.
Values may be sent and summed in bfloat16 or wider, within the bound.
A program may use at most 320 MiB of HBM per device.

```python
import math
import jax
import jax.numpy as jnp
import numpy as np
from jax import lax

SEP = 4096
B = 128
ANC = 16
MAXU = 6
GROUPS = 4
UNITS = 48
NSG = 16
WMAX = 768


def draw_ancestors(key, part):
    count_blocks = SEP // B
    noise = jax.random.randint(key, (GROUPS, NSG, count_blocks), 0, 4 * count_blocks)
    index = jnp.arange(count_blocks, dtype=jnp.int32)
    scores = (noise + index) * count_blocks + index
    chosen = lax.top_k(scores, ANC)[1]
    return jnp.sort(chosen, axis=-1).astype(jnp.int32)


def block_levels(rng, shape, shards, low, high):
    def one(dim, parts):
        heights = jax.random.uniform(jax.random.fold_in(jax.random.fold_in(rng, 6), dim), (parts,), jnp.float32, low / len(shards), high / len(shards))
        return jnp.repeat(jnp.exp(heights), shape[dim] // parts).reshape((-1,) + (1,) * (len(shape) - dim - 1))

    loudness = one(*shards[0])
    for cut in shards[1:]:
        loudness = loudness * one(*cut)
    return loudness


def profile(count, total, reach, skew):
    weights = [(1 << 20) // math.isqrt(standing ** skew) + 1 for standing in range(2, count + 1)]
    spare, counts = total - reach - (count - 1), [1] * (count - 1)
    while spare > 0:
        candidates = [i for i in range(count - 1) if counts[i] < reach]
        whole, left = sum([weights[i] for i in candidates]), spare
        for i in candidates:
            more = min(reach - counts[i], max(1, left * weights[i] // whole), spare)
            counts[i] = counts[i] + more
            spare = spare - more
    return np.array([reach] + counts)


def uneven_parts(stream_key, count, total, limit, lean):
    if count == 2:
        one = jax.random.randint(stream_key, (), max(1, total - limit), min(limit, total - 1) + 1)
        return jnp.stack([one, total - one])
    sizes = jnp.asarray(profile(count, total, limit, lean), jnp.int32)
    couples = (count - 1) // 2
    giver, receiver = sizes[1:1 + 2 * couples:2], sizes[2:2 + 2 * couples:2]
    room = jnp.minimum(giver - 1, limit - receiver)
    passed = jax.random.randint(jax.random.fold_in(stream_key, 1), (couples,), 0, 1 << 20) % (room + 1)
    sizes = sizes.at[1:1 + 2 * couples:2].set(giver - passed).at[2:2 + 2 * couples:2].set(receiver + passed)
    return sizes[jax.random.permutation(jax.random.fold_in(stream_key, 2), count)]


def scatter_about(stream_key, dims, deviation, most, split=(), held_as=jnp.bfloat16):
    array = jax.random.normal(stream_key, dims, jnp.float32) * deviation
    if len(split) > 0:
        array = block_levels(stream_key, dims, split, -0.22, 0.18) * array
    return jnp.clip(array, min=-most, max=most).astype(held_as)


def setup_inputs(seed: int = 0) -> dict:
    seeds = jax.random.split(jax.random.key(seed), 6)
    return {
        "sep_inv": scatter_about(seeds[0], (SEP, SEP), (ANC * B) ** -0.5, 0.125, ((0, 4), (1, 8))),
        "panels": scatter_about(seeds[1], (GROUPS, UNITS, ANC * B, B), 0.2, 1.1953125, ((0, 4), (1, 8))),
        "diag_inverse": scatter_about(seeds[2], (GROUPS, UNITS, WMAX, B), 1.0, 6.0, ((0, 4), (1, 8))),
        "widths": jax.vmap(lambda own: uneven_parts(own, NSG, UNITS, MAXU, 1))(jax.random.split(seeds[3], GROUPS)).reshape((GROUPS, NSG)).astype(jnp.int32),
        "ancestors": draw_ancestors(jax.random.fold_in(seeds[5], 71), 0),
    }


def reference(sep_inv, panels, diag_inverse, widths, ancestors):
    units = panels.shape[1]
    count_blocks = SEP // B
    tiles = sep_inv.astype(jnp.float32).reshape(count_blocks, B, count_blocks, B).transpose(0, 2, 1, 3)

    def per_group(group_args):
        panel_g, dinv_g, width_g, anc_g = group_args
        ends = jnp.cumsum(width_g).astype(jnp.int32)
        starts = ends - width_g
        position = jnp.arange(units, dtype=jnp.int32)
        owner = jnp.sum((ends[None, :] <= position[:, None]).astype(jnp.int32), axis=1).astype(jnp.int32)
        column = position - starts[owner]
        width_u = width_g[owner]
        blocks = anc_g[owner]
        padded = jnp.pad(panel_g, ((MAXU - 1, MAXU - 1), (0, 0), (0, 0)))

        def per_unit(unit_idx):
            chosen = blocks[unit_idx]
            picked = tiles[chosen[:, None], chosen[None, :]]
            panel_u = panel_g[unit_idx].astype(jnp.float32).reshape(ANC, B, B)
            product = jnp.einsum('abij,bjc->aic', picked, panel_u).reshape(ANC * B, B)
            result_x = (-product).astype(jnp.bfloat16)
            start_at = (unit_idx + MAXU - 1 - column[unit_idx]).astype(jnp.int32)
            related = lax.dynamic_slice_in_dim(padded, start_at, MAXU, 0)
            inner = jnp.einsum('jrb,rc->jbc', related.astype(jnp.float32), result_x.astype(jnp.float32))
            keep = (jnp.arange(MAXU, dtype=jnp.int32) < width_u[unit_idx]).astype(jnp.float32)
            diag_block = (dinv_g[unit_idx].astype(jnp.float32).reshape(MAXU, B, B) - inner) * keep[:, None, None]
            return result_x, diag_block.reshape(MAXU * B, B).astype(jnp.bfloat16)

        return lax.map(per_unit, jnp.arange(units, dtype=jnp.int32))

    off_diag, diag_panels = lax.map(per_group, (panels, diag_inverse, widths, ancestors))
    return off_diag, diag_panels
```

```python
import functools
import jax
import jax.numpy as jnp
from jax import lax
from jax.experimental import pallas as pl
from jax.experimental.pallas import tpu as pltpu
from jax.sharding import PartitionSpec as P

PIECES = 2


def halo_2(cells, width, axis):
    count = lax.axis_size(axis)
    ends = count - 1
    head = lax.slice_in_dim(cells, 0, width, axis=0)
    tail = lax.slice_in_dim(cells, cells.shape[0] - width, cells.shape[0], axis=0)
    before = lax.ppermute(tail, axis, [(i, (i + 1) % count) for i in range(ends)])
    after = lax.ppermute(head, axis, [((i + 1) % count, i) for i in range(ends)])
    return jnp.concatenate([before, cells, after], axis=0)


def spread_kernel(tiles, anc_tiles, block, where_ref, panel_ref, out_ref):
    unit = pl.program_id(0)
    for t in range(tiles):
        at = where_ref[unit, t]
        row = pl.multiple_of(jnp.minimum(at, anc_tiles - 1) * block, block)
        tile = panel_ref[pl.ds(row, block), :]
        out_ref[t * block : (t + 1) * block, :] = jnp.where(at < anc_tiles, tile, jnp.zeros_like(tile))


def product_kernel(parts, part_cols, sep_ref, spread_ref, out_ref):
    rows = jnp.concatenate([sep_ref[d] for d in range(parts)], axis=1)
    total = jnp.dot(rows, spread_ref[...], preferred_element_type=jnp.float32)
    out_ref[...] = (-total).astype(out_ref.dtype)


def result_kernel(
    anc_tiles, max_tiles, block, per_part, per_piece,
    chosen_ref, start_ref, width_ref, *refs
):
    pieces = refs[:PIECES]
    ext_ref, dinv_ref, off_ref, diag_ref = refs[PIECES:]
    unit = pl.program_id(0)
    for a in range(anc_tiles):
        tile = chosen_ref[unit, a]
        inside = lax.rem(tile, per_part)
        piece = lax.div(inside, per_piece)
        index = lax.div(tile, per_part) * per_piece + lax.rem(inside, per_piece)
        row = pl.multiple_of(index * block, block)
        value = pieces[0][pl.ds(row, block), :]
        for p in range(1, PIECES):
            value = jnp.where(piece == p, pieces[p][pl.ds(row, block), :], value)
        off_ref[a * block : (a + 1) * block, :] = value
    start = start_ref[unit]
    width = width_ref[unit]
    related = jnp.concatenate([ext_ref[start + j] for j in range(max_tiles)], axis=1)
    inner = lax.dot_general(
        off_ref[...], related, (((0,), (0,)), ((), ())), preferred_element_type=jnp.float32
    )
    for j in range(max_tiles):
        rows = slice(j * block, (j + 1) * block)
        value = dinv_ref[rows, :].astype(jnp.float32) - inner[:, rows].T
        diag_ref[rows, :] = jnp.where(j < width, value, jnp.zeros_like(value)).astype(diag_ref.dtype)


def on_device(sep_inv, panels, diag_inverse, widths, ancestors):
    group_count = lax.axis_size("grp")
    device_count = lax.axis_size("dev")
    rows_local, cols_local = sep_inv.shape
    local_units, anc_rows, block = panels.shape[1:]
    anc_tiles = anc_rows // block
    max_tiles = diag_inverse.shape[2] // block
    sep_order = group_count * rows_local
    count_blocks = sep_order // block
    columns = local_units * block
    piece_rows = rows_local // PIECES
    gathered = [
        lax.all_gather(
            lax.slice_in_dim(sep_inv, p * piece_rows, (p + 1) * piece_rows, axis=0),
            ("grp", "dev"), axis=0, tiled=False,
        ).reshape(group_count, device_count, piece_rows, cols_local)
        for p in range(PIECES)
    ]
    extended = halo_2(panels[0], max_tiles - 1, "dev")

    width_row = widths[0]
    anc_table = ancestors[0]
    supernodes = width_row.shape[0]
    ends = jnp.cumsum(width_row)
    starts = ends - width_row
    position = lax.axis_index("dev") * local_units + jnp.arange(local_units, dtype=jnp.int32)
    owner = jnp.sum((ends[None, :] <= position[:, None]).astype(jnp.int32), axis=1)
    one_hot = (jnp.arange(supernodes, dtype=jnp.int32)[None, :] == owner[:, None]).astype(jnp.int32)
    column = position - jnp.sum(one_hot * starts[None, :], axis=1)
    width_unit = jnp.sum(one_hot * width_row[None, :], axis=1)
    chosen = jnp.sum(one_hot[:, :, None] * anc_table[None, :, :], axis=1)
    start_at = jnp.arange(local_units, dtype=jnp.int32) + (max_tiles - 1) - column
    tile_ids = jnp.arange(count_blocks, dtype=jnp.int32)
    hit = chosen[:, :, None] == tile_ids[None, None, :]
    slot = jnp.arange(anc_tiles, dtype=jnp.int32)[None, :, None]
    where_at = jnp.min(jnp.where(hit, slot, anc_tiles), axis=1).astype(jnp.int32)

    spread = pl.pallas_call(
        functools.partial(spread_kernel, count_blocks, anc_tiles, block),
        out_shape=jax.ShapeDtypeStruct((sep_order, columns), jnp.bfloat16),
        grid_spec=pltpu.PrefetchScalarGridSpec(
            num_scalar_prefetch=1,
            grid=(local_units,),
            in_specs=[pl.BlockSpec((None, anc_rows, block), lambda u, w: (u, 0, 0))],
            out_specs=pl.BlockSpec((sep_order, block), lambda u, w: (0, u)),
        ),
        cost_estimate=pl.CostEstimate(
            flops=sep_order * columns, transcendentals=0,
            bytes_accessed=4 * sep_order * columns,
        ),
        name="spread",
    )(where_at, panels[0])

    step_rows = min(256, piece_rows)
    steps = piece_rows // step_rows

    def product(piece):
        return pl.pallas_call(
            functools.partial(product_kernel, device_count, cols_local),
            out_shape=jax.ShapeDtypeStruct((group_count * piece_rows, columns), jnp.bfloat16),
            grid=(group_count, steps),
            in_specs=[
                pl.BlockSpec((None, device_count, step_rows, cols_local), lambda g, r: (g, 0, r, 0)),
                pl.BlockSpec((sep_order, columns), lambda g, r: (0, 0)),
            ],
            out_specs=pl.BlockSpec((step_rows, columns), lambda g, r: (g * steps + r, 0)),
            cost_estimate=pl.CostEstimate(
                flops=2 * group_count * piece_rows * sep_order * columns, transcendentals=0,
                bytes_accessed=2 * group_count * piece_rows * sep_order + 2 * sep_order * columns,
            ),
            name="product",
        )(piece, spread)

    products = [product(piece) for piece in gathered]
    piece_order = group_count * piece_rows
    off_diag, diag_panels = pl.pallas_call(
        functools.partial(
            result_kernel, anc_tiles, max_tiles, block, rows_local // block, piece_rows // block
        ),
        out_shape=(
            jax.ShapeDtypeStruct((local_units, anc_rows, block), jnp.bfloat16),
            jax.ShapeDtypeStruct((local_units, max_tiles * block, block), jnp.bfloat16),
        ),
        grid_spec=pltpu.PrefetchScalarGridSpec(
            num_scalar_prefetch=3,
            grid=(local_units,),
            in_specs=[pl.BlockSpec((piece_order, block), lambda u, *_: (0, u))] * PIECES
            + [
                pl.BlockSpec(extended.shape, lambda u, *_: (0, 0, 0)),
                pl.BlockSpec((None, max_tiles * block, block), lambda u, *_: (u, 0, 0)),
            ],
            out_specs=[
                pl.BlockSpec((None, anc_rows, block), lambda u, *_: (u, 0, 0)),
                pl.BlockSpec((None, max_tiles * block, block), lambda u, *_: (u, 0, 0)),
            ],
        ),
        cost_estimate=pl.CostEstimate(
            flops=2 * local_units * anc_rows * block * block * max_tiles, transcendentals=0,
            bytes_accessed=4 * sep_order * columns,
        ),
        name="result",
    )(chosen, start_at, width_unit, *products, extended, diag_inverse[0])
    return (off_diag[None], diag_panels[None])


def solution(mesh):
    placed = (
        P("grp", "dev"),
        P("grp", "dev", None, None),
        P("grp", "dev", None, None),
        P("grp", None),
        P("grp", None, None),
    )
    return jax.shard_map(
        on_device,
        mesh=mesh,
        in_specs=placed,
        out_specs=(P("grp", "dev", None, None), P("grp", "dev", None, None)),
        check_vma=False,
    )
```
